32 devices in a mesh: wa: 8 (over z, y), ba: 4 (over x, core).
Axes of the slice: x: 2, y: 2, z: 4, core: 2. Of those that a mesh axis runs over, the one named last changes fastest.
Arguments:
- latent: float32 [16, 8, 1024], P('ba', None, 'wa'), parts along dimension 0, may hold values from -12 to 12
- noise: float32 [2, 16, 8, 1024], P(None, 'ba', None, 'wa'), parts along dimension 1, may hold values from -6 to 6
- offsets: int32 [16], P('wa'), may hold values from 0 to 63
- anchors: int32 [2], replicated, may hold values from 0 to 15
- guidance: float32 [1], replicated, may hold values from 0.4 to 0.8
- w_in: bfloat16 [320, 36], replicated, may hold values from -1 to 1
- w_mid: bfloat16 [320, 320], replicated, may hold values from -0.3125 to 0.3125
- w_out: bfloat16 [36, 320], replicated, may hold values from -0.109375 to 0.109375
- t_embed: float32 [2, 320], replicated, may hold values from -6 to 6
- w_feat: float32 [64, 4], replicated, may hold values from -3 to 3
Outputs:
- denoised: float32 [16, 8, 1024], P('ba', None, 'wa'), parts along dimension 0
The draws below stay inside these ranges and needn't reach their ends.
There are 4 independent parts, one for each index of `ba`. The reference program is written for one: setup_inputs(seed, part) draws one part's arguments, and reference() takes and returns one part's arrays. A program takes and returns all parts, laid end to end along the dimension named above; an argument that names none is the same for every part. Nothing has to cross between parts.
All inputs are finite; a program needn't handle non-finite values.
Results may differ from the reference program's by a relative error of at most 0.0065.
Values sent between devices are 32-bit elements; how exact they have to be, the bound alone decides.
A program may use at most 64 MiB of HBM per device.

```python
import math
import jax
import jax.numpy as jnp
from jax import lax

C = 4
HID = 320
FEAT = 64
H = 8
WIN = 128
STRIDE = 64
STEPS = 2
NWIN = 16
W = 1024


def draw_latent(key, part):
    base_key = jax.random.fold_in(key, 7)
    normal_key = jax.random.fold_in(base_key, 0)
    columns = jnp.arange(W, dtype=jnp.float32)
    rising = 2.0 ** (columns / W)
    values = jax.random.normal(normal_key, (C, H, W), jnp.float32)
    return jnp.clip(values * rising, -12.0, 12.0)


def place_ends(values, own_key, smallest, largest):
    spot = [jax.random.randint(jax.random.fold_in(own_key, axis), (), 0, length) for axis, length in enumerate(values.shape)]
    longest = values.shape.index(max(values.shape))
    neighbour = spot[:longest] + [(spot[longest] + 1) % values.shape[longest]] + spot[longest + 1:]
    return values.at[tuple(spot)].set(smallest).at[tuple(neighbour)].set(largest)


def levels(stream_key, extent, cuts, low, top_value):
    def one(dim, parts):
        steps = jax.random.uniform(jax.random.fold_in(jax.random.fold_in(stream_key, 6), dim), (parts,), jnp.float32, low / len(cuts), top_value / len(cuts))
        return jnp.repeat(jnp.exp(steps), extent[dim] // parts).reshape((-1,) + (1,) * (len(extent) - dim - 1))

    loudness = one(*cuts[0])
    for cut in cuts[1:]:
        loudness = loudness * one(*cut)
    return loudness


def normal_values(stream_key, extent, scale, bound, shards=(), kind=jnp.bfloat16):
    values = jax.random.normal(stream_key, extent, jnp.float32) * scale
    if len(shards) > 0:
        values = levels(stream_key, extent, shards, -0.22, 0.18) * values
    return jnp.clip(values, min=-bound, max=bound).astype(kind)


def setup_inputs(seed: int = 0, part: int = 0) -> dict:
    key_list = jax.random.split(jax.random.key(seed), 11)
    own_keys = jax.random.split(jax.random.fold_in(key_list[10], part), 11)
    latent = draw_latent(jax.random.fold_in(jax.random.fold_in(key_list[10], part), 71), part)
    noise = normal_values(own_keys[1], (STEPS, C, H, W), 1.0, 6.0, ((3, 8),), jnp.float32)
    offsets = place_ends(jax.random.randint(key_list[2], (NWIN,), 0, STRIDE), jax.random.fold_in(key_list[2], 1), 0, STRIDE - 1).astype(jnp.int32)
    anchors = jax.random.randint(key_list[3], (STEPS,), 0, NWIN).astype(jnp.int32)
    guidance = jnp.clip(jax.random.uniform(key_list[4], (1,), jnp.float32, 0.4, 0.8), 0.4, 0.8)
    w_in = normal_values(key_list[5], (HID, 9 * C), (9 * C) ** -0.5, 1.0)
    w_mid = normal_values(key_list[6], (HID, HID), HID ** -0.5, 0.3125)
    w_out = normal_values(key_list[7], (9 * C, HID), (9 * HID) ** -0.5, 0.109375)
    t_embed = normal_values(key_list[8], (STEPS, HID), 1.0, 6.0, (), jnp.float32)
    w_feat = normal_values(key_list[9], (FEAT, C), C ** -0.5, 3.0, (), jnp.float32)
    return {"latent": latent, "noise": noise, "offsets": offsets, "anchors": anchors, "guidance": guidance, "w_in": w_in, "w_mid": w_mid, "w_out": w_out, "t_embed": t_embed, "w_feat": w_feat}


TAP_SHIFTS = ((-1, -1), (-1, 0), (-1, 1), (0, -1), (0, 0), (0, 1), (1, -1), (1, 0), (1, 1))
CUMULATIVE_ALPHA = (0.35, 0.55, 0.72, 0.85, 0.93)
STABILITY = 1e-06

def plan(number):
    current = CUMULATIVE_ALPHA[number]
    following = CUMULATIVE_ALPHA[number + 1]
    spread = 0.3 * math.sqrt(1.0 - following)
    return (math.sqrt(current), math.sqrt(1.0 - current), math.sqrt(following), math.sqrt(1.0 - following - spread * spread), spread)

def tapped(field):
    height, columns = (field.shape[-2], field.shape[-1])
    padding = [(0, 0)] * (field.ndim - 2) + [(1, 1), (1, 1)]
    padded = jnp.pad(field, padding)
    return jnp.stack([padded[..., 1 + down_by:1 + down_by + height, 1 + right_by:1 + right_by + columns] for down_by, right_by in TAP_SHIFTS])

def denoise(window, w_in, w_mid, w_out, embedding):
    channels, height, columns = window.shape
    stacked = tapped(window.astype(jnp.bfloat16)).reshape(9 * channels, height * columns)
    hidden_in = jnp.dot(w_in, stacked, preferred_element_type=jnp.float32) + embedding[:, None]
    activated = jax.nn.silu(hidden_in).astype(jnp.bfloat16)
    middle = jnp.dot(w_mid, activated, preferred_element_type=jnp.float32)
    joined = (hidden_in + jax.nn.silu(middle)).astype(jnp.bfloat16)
    outward = jnp.dot(w_out, joined, preferred_element_type=jnp.float32).reshape(9, channels, height, columns)
    padded = jnp.pad(outward, ((0, 0), (0, 0), (1, 1), (1, 1)))
    result = jnp.zeros((channels, height, columns), jnp.float32)
    for index, (down_by, right_by) in enumerate(TAP_SHIFTS):
        result = result + padded[index, :, 1 + down_by:1 + down_by + height, 1 + right_by:1 + right_by + columns]
    return result

def clean_of(windows, w_in, w_mid, w_out, embedding, now_a, now_s):
    predicted = jax.vmap(denoise, (0, None, None, None, None))(windows, w_in, w_mid, w_out, embedding)
    cleaned = (windows - now_s * predicted) / now_a
    return (cleaned, predicted)

def percept(cleaned, w_feat):
    return jax.nn.silu(jnp.einsum('fc,chw->fhw', w_feat, cleaned, precision=lax.Precision.HIGHEST))

def mismatch(cleaned, anchor_percept, w_feat):
    difference = percept(cleaned, w_feat) - anchor_percept
    return 0.5 * jnp.sum(difference * difference) / w_feat.shape[0]

def finish_gradient(cleaned, pullback, anchor_percept, w_feat):
    clean_grad = jax.vmap(jax.grad(mismatch), (0, None, None))(cleaned, anchor_percept, w_feat)
    return pullback(clean_grad)[0]

def advance(windows, gradient, predicted, scale, now_a, now_s, next_a, direction):
    return next_a * (windows - scale * gradient - now_s * predicted) / now_a + direction * predicted

def reference(latent, noise, offsets, anchors, guidance, w_in, w_mid, w_out, t_embed, w_feat):
    channels, height, width = latent.shape
    window_count = offsets.shape[0]
    per_block = WIN // STRIDE
    starts = jnp.arange(window_count, dtype=jnp.int32) * STRIDE + offsets
    positions = jnp.arange(width + WIN, dtype=jnp.int32)
    inside = (positions[None, :] >= starts[:, None]) & (positions[None, :] < starts[:, None] + WIN)
    cover = lax.optimization_barrier(jnp.sum(inside.astype(jnp.float32), axis=0))
    counts = cover[:width].at[:WIN].add(cover[width:])
    block_starts = starts.reshape(window_count // per_block, per_block)
    state = latent
    for number in range(STEPS):
        now_a, now_s, next_a, direction, spread = plan(number)
        embedding = t_embed[number]
        padded_state = jnp.concatenate([state, state[:, :, :WIN]], axis=2)

        def cut_window(root):
            return lax.dynamic_slice_in_dim(padded_state, root, WIN, 2)

        def forward(roots):
            windows = jax.vmap(cut_window)(roots)
            return clean_of(windows, w_in, w_mid, w_out, embedding, now_a, now_s)[0]
        cleaned_all = lax.map(forward, block_starts).reshape(window_count, channels, height, WIN)
        anchor_clean = lax.dynamic_index_in_dim(cleaned_all, anchors[number], 0, keepdims=False)
        anchor_percept = percept(anchor_clean, w_feat)

        def backward(roots):
            windows = jax.vmap(cut_window)(roots)

            def cleaning(inputs):
                return clean_of(inputs, w_in, w_mid, w_out, embedding, now_a, now_s)
            cleaned, pullback, predicted = jax.vjp(cleaning, windows, has_aux=True)
            gradient = finish_gradient(cleaned, pullback, anchor_percept, w_feat)
            return (gradient, predicted, jnp.sum(gradient * gradient))
        gradients, predictions, squares = lax.map(backward, block_starts)
        mean_square = jnp.sum(squares) / (window_count * channels * height * WIN)
        scale = guidance[0] * lax.rsqrt(mean_square + STABILITY)
        windows = jax.vmap(cut_window)(starts)
        advanced = advance(windows, gradients.reshape(windows.shape), predictions.reshape(windows.shape), scale, now_a, now_s, next_a, direction)

        def place(summed, element):
            root, piece = element
            current = lax.dynamic_slice_in_dim(summed, root, WIN, 2)
            return (lax.dynamic_update_slice_in_dim(summed, current + piece, root, 2), None)
        summed = lax.scan(place, jnp.zeros((channels, height, width + WIN), jnp.float32), (starts, advanced))[0]
        blended = summed[:, :, :width].at[:, :, :WIN].add(summed[:, :, width:])
        state = blended / counts + spread * noise[number]
    return state
```

```python
import functools
import math

import jax
import jax.numpy as jnp
from jax import lax
from jax.experimental import pallas as pl
from jax.experimental.pallas import tpu as pltpu
from jax.sharding import PartitionSpec as P

WIN = 128
STRIDE = 64
CHUNK = 256

TAP_SHIFTS = ((-1, -1), (-1, 0), (-1, 1), (0, -1), (0, 0), (0, 1), (1, -1), (1, 0), (1, 1))
CUMULATIVE_ALPHA = (0.35, 0.55, 0.72, 0.85, 0.93)
STABILITY = 1e-06
F32 = jnp.float32
BF16 = jnp.bfloat16


def plan(number):
    current = CUMULATIVE_ALPHA[number]
    following = CUMULATIVE_ALPHA[number + 1]
    spread = 0.3 * math.sqrt(1.0 - following)
    return (
        math.sqrt(current),
        math.sqrt(1.0 - current),
        math.sqrt(following),
        math.sqrt(1.0 - following - spread * spread),
        spread,
    )


def mm(a, b):
    return jnp.dot(a, b, preferred_element_type=F32)


def mm_nt(a, b):
    return lax.dot_general(a, b, (((1,), (1,)), ((), ())), preferred_element_type=F32)


def silu_pair(v):
    s = 0.5 * jnp.tanh(0.5 * v) + 0.5
    a = v * s
    return a, s + a * (1.0 - s)


def kernel(
    n, steps, per_dev, channels, height, width, hid, feat,
    latent_ref, noise_ref, offsets_ref, anchors_ref, guidance_ref,
    w_in_ref, w_mid_ref, w_out_ref, t_embed_ref, w_feat_ref,
    out_ref,
    wi, wit, wo, wot, wmt, emb, wfb,
    taps, outward, deriv_h, deriv_m, clean_ref, per_a, per_d, dclean_ref,
    init_src, init_dst, cover_src, cover_dst,
    anchor_buf, square_buf, own_src, own_dst, spill_src, spill_dst,
    init_send, init_recv, anchor_send, anchor_recv, square_send, square_recv, edge_send, edge_recv,
):
    me = lax.axis_index("wa")
    right, left = lax.rem(me + 1, n), lax.rem(me + n - 1, n)
    rows = per_dev * channels
    flat = height * width
    nine = len(TAP_SHIFTS)

    barrier = pltpu.get_barrier_semaphore()

    def greet(d, carry):
        pl.semaphore_signal(
            barrier, inc=1, device_id={"wa": lax.rem(me + d, n)},
            device_id_type=pl.DeviceIdType.MESH,
        )
        return carry

    lax.fori_loop(1, n, greet, 0)

    def remote(src, dst, send_sem, recv_sem, target):
        return pltpu.make_async_remote_copy(
            src_ref=src, dst_ref=dst, send_sem=send_sem, recv_sem=recv_sem,
            device_id={"wa": target}, device_id_type=pl.DeviceIdType.MESH,
        )

    def to_all(buf, send_sem, recv_sem):
        def one(d, carry):
            remote(buf.at[0], buf.at[d], send_sem, recv_sem, lax.rem(me + d, n)).start()
            return carry

        lax.fori_loop(1, n, one, 0)

    def await_all(buf, sem):
        rest = buf.at[pl.ds(1, n - 1)]
        pltpu.make_async_copy(rest, rest, sem).wait()

    lane = lax.broadcasted_iota(jnp.int32, (rows, width), 1)
    row = lax.broadcasted_iota(jnp.int32, (rows, width), 0)
    first = row < channels
    row_all = lax.broadcasted_iota(jnp.int32, (rows, flat), 0)
    starts = [offsets_ref[i] + i * STRIDE for i in range(per_dev)]
    start_row = jnp.where(first, starts[0], starts[1])
    keep = lane >= start_row

    def tiles(value):
        return [value[:, h * width : (h + 1) * width] for h in range(height)]

    def joined_tiles(parts):
        return jnp.concatenate(parts, axis=1)

    def from_right(x):
        return jnp.where(lane == width - 1, 0.0, pltpu.roll(x, width - 1, 1))

    def from_left(x):
        return jnp.where(lane == 0, 0.0, pltpu.roll(x, 1, 1))

    def expand(parts, sign):
        moved = {0: parts, 1: [from_right(p) for p in parts], -1: [from_left(p) for p in parts]}
        zero = jnp.zeros((rows, width), F32)
        blocks = []
        for down, across in TAP_SHIFTS:
            source = moved[sign * across]
            blocks.append(
                joined_tiles(
                    [
                        source[h + sign * down] if 0 <= h + sign * down < height else zero
                        for h in range(height)
                    ]
                )
            )
        return jnp.concatenate(blocks, axis=0).astype(BF16)

    def collapse(ref, sign):
        result = []
        for h in range(height):
            sums = {}
            for k, (down, across) in enumerate(TAP_SHIFTS):
                source = h + sign * down
                if 0 <= source < height:
                    piece = ref[k * rows : (k + 1) * rows, source * width : (source + 1) * width]
                    key = sign * across
                    sums[key] = sums[key] + piece if key in sums else piece
            result.append(sums[0] + from_right(sums[1]) + from_left(sums[-1]))
        return result

    def half_swap(x):
        return pltpu.roll(x, channels, 0)

    for h in range(height):
        cols = slice(h * width, (h + 1) * width)
        init_src[0:channels, cols] = latent_ref[:, h, :]
        for s in range(steps - 1):
            init_src[(s + 1) * channels : (s + 2) * channels, cols] = noise_ref[s, :, h, :]
    own_cover = jnp.zeros((rows, width), F32)
    for i in range(per_dev):
        own_cover = own_cover + (lane >= starts[i]).astype(F32)
    spill_cover = per_dev - own_cover
    cover_src[0] = own_cover
    cover_src[1] = spill_cover

    pl.semaphore_wait(barrier, n - 1)
    init_copy = remote(init_src, init_dst, init_send.at[0], init_recv.at[0], left)
    cover_left = remote(cover_src.at[0], cover_dst.at[0], init_send.at[1], init_recv.at[1], left)
    cover_right = remote(cover_src.at[1], cover_dst.at[1], init_send.at[2], init_recv.at[2], right)
    init_copy.start()
    cover_left.start()
    cover_right.start()

    w_in = w_in_ref[...]
    w_out = w_out_ref[...]
    small = nine * channels
    eye_r = lax.broadcasted_iota(jnp.int32, (hid, hid), 0)
    eye_c = lax.broadcasted_iota(jnp.int32, (hid, hid), 1)
    eye = eye_r == eye_c
    eye_b = jnp.where(eye, 1.0, 0.0).astype(BF16)
    wmt[...] = mm_nt(eye_b, w_mid_ref[...]).astype(BF16)
    w_out_t = mm_nt(eye_b, w_out).astype(BF16)
    for i in range(per_dev):
        def hot(a, b):
            return jnp.where((a // channels) * rows + i * channels + a % channels == b, 1.0, 0.0).astype(BF16)

        spot = hot(
            lax.broadcasted_iota(jnp.int32, (small, nine * rows), 0),
            lax.broadcasted_iota(jnp.int32, (small, nine * rows), 1),
        )
        spot_t = hot(
            lax.broadcasted_iota(jnp.int32, (nine * rows, small), 1),
            lax.broadcasted_iota(jnp.int32, (nine * rows, small), 0),
        )
        wi[i] = mm(w_in, spot).astype(BF16)
        wit[i] = mm_nt(spot_t, w_in).astype(BF16)
        wo[i] = mm(spot_t, w_out).astype(BF16)
        wot[i] = mm(w_out_t, spot).astype(BF16)
    for s in range(steps):
        column = jnp.sum(jnp.where(eye, t_embed_ref[s : s + 1, :], 0.0), axis=1, keepdims=True)
        emb[s] = jnp.broadcast_to(column, (hid, WIN))
    for c in range(channels):
        wfb[c] = jnp.broadcast_to(w_feat_ref[:, c : c + 1], (feat, width))

    cover_left.wait()
    cover_right.wait()
    count_own = own_cover + cover_dst[1]
    count_next = cover_dst[0] + spill_cover
    init_copy.wait()

    def doubled(value):
        return jnp.concatenate([value] * per_dev, axis=0)

    state = tiles(doubled(init_src[0:channels, :]))
    state_next = tiles(doubled(init_dst[0:channels, :]))

    for s in range(steps):
        now_a, now_s, next_a, direction, spread = plan(s)
        last = s == steps - 1

        window = []
        for h in range(height):
            cut = [
                pltpu.roll(jnp.where(lane >= start, state[h], state_next[h]), width - start, 1)
                for start in starts
            ]
            window.append(jnp.where(first, cut[0], cut[1]))
        taps[...] = expand(window, 1)

        def forward(j, carry):
            cols = pl.ds(pl.multiple_of(j * CHUNK, CHUNK), CHUNK)
            stacked = taps[:, cols]
            shift = jnp.concatenate([emb[s]] * (CHUNK // WIN), axis=1)
            total = None
            for i in range(per_dev):
                hidden = mm(wi[i], stacked) + shift
                act, slope = silu_pair(hidden)
                deriv_h[i, :, cols] = slope
                middle = mm(w_mid_ref[...], act.astype(BF16))
                act2, slope2 = silu_pair(middle)
                deriv_m[i, :, cols] = slope2
                piece = mm(wo[i], (hidden + act2).astype(BF16))
                total = piece if total is None else total + piece
            outward[:, cols] = total
            return carry

        lax.fori_loop(0, flat // CHUNK, forward, 0)

        predicted = collapse(outward, 1)
        cleaned = [(window[h] - now_s * predicted[h]) * (1.0 / now_a) for h in range(height)]
        clean_all = joined_tiles(cleaned)
        clean_ref[...] = clean_all
        chosen = jnp.where(row_all // channels + me * per_dev == anchors_ref[s], clean_all, 0.0)
        chosen = chosen + half_swap(chosen)
        anchor_buf[s, 0] = chosen[0:channels, :]
        to_all(anchor_buf.at[s], anchor_send.at[s], anchor_recv.at[s])

        def percept_of(source, base):
            value = wfb[0] * source[base : base + 1, :]
            for c in range(1, channels):
                value = value + wfb[c] * source[base + c : base + c + 1, :]
            return value

        def features(h, carry):
            cols = pl.ds(pl.multiple_of(h * width, width), width)
            source = clean_ref[:, cols]
            for i in range(per_dev):
                act, slope = silu_pair(percept_of(source, i * channels))
                per_a[i, :, cols] = act
                per_d[i, :, cols] = slope
            return carry

        lax.fori_loop(0, height, features, 0)

        await_all(anchor_buf.at[s], anchor_recv.at[s])

        def backward_features(h, carry):
            cols = pl.ds(pl.multiple_of(h * width, width), width)
            anchor = anchor_buf[s, 0, :, cols]
            for d in range(1, n):
                anchor = anchor + anchor_buf[s, d, :, cols]
            anchor_act = silu_pair(percept_of(anchor, 0))[0]
            lines = []
            for i in range(per_dev):
                slope = (per_a[i, :, cols] - anchor_act) * (1.0 / feat) * per_d[i, :, cols]
                for c in range(channels):
                    lines.append(jnp.sum(wfb[c] * slope, axis=0, keepdims=True))
            dclean_ref[:, cols] = jnp.concatenate(lines, axis=0)
            return carry

        lax.fori_loop(0, height, backward_features, 0)

        dclean = tiles(dclean_ref[...])
        taps[...] = expand([(-now_s / now_a) * d for d in dclean], -1)

        def backward(j, carry):
            cols = pl.ds(pl.multiple_of(j * CHUNK, CHUNK), CHUNK)
            stacked = taps[:, cols]
            total = None
            for i in range(per_dev):
                d_joined = mm(wot[i], stacked).astype(BF16).astype(F32)
                d_middle = (d_joined * deriv_m[i, :, cols]).astype(BF16)
                d_act = mm(wmt[...], d_middle).astype(BF16).astype(F32)
                d_hidden = (d_joined + d_act * deriv_h[i, :, cols]).astype(BF16)
                piece = mm(wit[i], d_hidden)
                total = piece if total is None else total + piece
            outward[:, cols] = total.astype(BF16).astype(F32)
            return carry

        lax.fori_loop(0, flat // CHUNK, backward, 0)

        through = collapse(outward, -1)
        gradient = [
            dclean[h] * (1.0 / now_a) + through[h].astype(BF16).astype(F32) for h in range(height)
        ]
        square = gradient[0] * gradient[0]
        for h in range(1, height):
            square = square + gradient[h] * gradient[h]
        square_buf[s, 0] = square
        to_all(square_buf.at[s], square_send.at[s], square_recv.at[s])

        def placed(x):
            moved = jnp.where(first, pltpu.roll(x, starts[0], 1), pltpu.roll(x, starts[1], 1))
            own = jnp.where(keep, moved, 0.0)
            over = moved - own
            return own + half_swap(own), over + half_swap(over)

        own_parts, spill_parts = [], []
        for h in range(height):
            base = (next_a / now_a) * (window[h] - now_s * predicted[h]) + direction * predicted[h]
            base_own, base_over = placed(base)
            grad_own, grad_over = placed(gradient[h])
            own_parts.append(jnp.where(first, base_own, grad_own))
            spill_parts.append(jnp.where(first, base_over, grad_over))
        spill_src[s] = joined_tiles(spill_parts)
        to_right = remote(spill_src.at[s], spill_dst.at[s], edge_send.at[2 * s], edge_recv.at[2 * s], right)
        to_right.start()
        if not last:
            own_src[s] = joined_tiles(own_parts)
            to_left = remote(own_src.at[s], own_dst.at[s], edge_send.at[2 * s + 1], edge_recv.at[2 * s + 1], left)
            to_left.start()

        def merged(own, spill, coef, count, noise):
            both = own + spill
            swapped = half_swap(both)
            base = jnp.where(first, both, swapped)
            grad = jnp.where(first, swapped, both)
            return (base - coef * grad) / count + spread * noise

        await_all(square_buf.at[s], square_recv.at[s])
        square = square_buf[s, 0]
        for d in range(1, n):
            square = square + square_buf[s, d]
        mean = jnp.sum(jnp.sum(square, axis=0, keepdims=True), axis=1, keepdims=True) * (
            1.0 / (n * rows * flat)
        )
        coef = (next_a / now_a) * guidance_ref[0] * lax.rsqrt(
            jnp.broadcast_to(mean, (rows, width)) + STABILITY
        )
        to_right.wait()
        spill = tiles(spill_dst[s])
        if last:
            for h in range(height):
                noise = doubled(noise_ref[s, :, h, :])
                out_ref[:, h, :] = merged(own_parts[h], spill[h], coef, count_own, noise)[0:channels, :]
        else:
            to_left.wait()
            noise_own = tiles(doubled(init_src[(s + 1) * channels : (s + 2) * channels, :]))
            noise_next = tiles(doubled(init_dst[(s + 1) * channels : (s + 2) * channels, :]))
            arrived = tiles(own_dst[s])
            state = [
                merged(own_parts[h], spill[h], coef, count_own, noise_own[h]) for h in range(height)
            ]
            state_next = [
                merged(arrived[h], spill_parts[h], coef, count_next, noise_next[h])
                for h in range(height)
            ]

    for s in range(steps):
        await_all(anchor_buf.at[s], anchor_send.at[s])
        await_all(square_buf.at[s], square_send.at[s])


def local(n, latent, noise, offsets, anchors, guidance, w_in, w_mid, w_out, t_embed, w_feat):
    channels, height, width = latent.shape
    per_dev = offsets.shape[0]
    steps = t_embed.shape[0]
    hid = w_mid.shape[0]
    feat = w_feat.shape[0]
    rows = per_dev * channels
    assert width == WIN and per_dev == 2
    flat = height * width
    tall = len(TAP_SHIFTS) * rows
    vmem = pl.BlockSpec(memory_space=pltpu.VMEM)
    smem = pl.BlockSpec(memory_space=pltpu.SMEM)
    dma = pltpu.SemaphoreType.DMA
    return pl.pallas_call(
        functools.partial(kernel, n, steps, per_dev, channels, height, width, hid, feat),
        out_shape=jax.ShapeDtypeStruct(latent.shape, F32),
        in_specs=[vmem, vmem, smem, smem, smem, vmem, vmem, vmem, vmem, vmem],
        out_specs=vmem,
        scratch_shapes=[
            pltpu.VMEM((per_dev, hid, tall), BF16),
            pltpu.VMEM((per_dev, tall, hid), BF16),
            pltpu.VMEM((per_dev, tall, hid), BF16),
            pltpu.VMEM((per_dev, hid, tall), BF16),
            pltpu.VMEM((hid, hid), BF16),
            pltpu.VMEM((steps, hid, WIN), F32),
            pltpu.VMEM((channels, feat, width), F32),
            pltpu.VMEM((tall, flat), BF16),
            pltpu.VMEM((tall, flat), F32),
            pltpu.VMEM((per_dev, hid, flat), F32),
            pltpu.VMEM((per_dev, hid, flat), F32),
            pltpu.VMEM((rows, flat), F32),
            pltpu.VMEM((per_dev, feat, flat), F32),
            pltpu.VMEM((per_dev, feat, flat), F32),
            pltpu.VMEM((rows, flat), F32),
            pltpu.VMEM((steps * channels, flat), F32),
            pltpu.VMEM((steps * channels, flat), F32),
            pltpu.VMEM((2, rows, width), F32),
            pltpu.VMEM((2, rows, width), F32),
            pltpu.VMEM((steps, n, channels, flat), F32),
            pltpu.VMEM((steps, n, rows, width), F32),
            pltpu.VMEM((steps, rows, flat), F32),
            pltpu.VMEM((steps, rows, flat), F32),
            pltpu.VMEM((steps, rows, flat), F32),
            pltpu.VMEM((steps, rows, flat), F32),
            dma((3,)),
            dma((3,)),
            dma((steps,)),
            dma((steps,)),
            dma((steps,)),
            dma((steps,)),
            dma((2 * steps,)),
            dma((2 * steps,)),
        ],
        compiler_params=pltpu.CompilerParams(
            collective_id=0, has_side_effects=True, vmem_limit_bytes=48 * 1024 * 1024
        ),
        name="panorama",
    )(latent, noise, offsets, anchors, guidance, w_in, w_mid, w_out, t_embed, w_feat)


def solution(mesh):
    return jax.shard_map(
        functools.partial(local, mesh.shape["wa"]),
        mesh=mesh,
        in_specs=(
            P("ba", None, "wa"),
            P(None, "ba", None, "wa"),
            P("wa"),
            P(),
            P(),
            P(),
            P(),
            P(),
            P(),
            P(),
        ),
        out_specs=P("ba", None, "wa"),
        check_vma=False,
    )
```

```python
import functools
import math

import jax
import jax.numpy as jnp
from jax import lax
from jax.experimental import pallas as pl
from jax.experimental.pallas import tpu as pltpu
from jax.sharding import PartitionSpec as P

WIN = 128
STRIDE = 64
CHUNK = 256
SIDE = 2

TAP_SHIFTS = ((-1, -1), (-1, 0), (-1, 1), (0, -1), (0, 0), (0, 1), (1, -1), (1, 0), (1, 1))
CUMULATIVE_ALPHA = (0.35, 0.55, 0.72, 0.85, 0.93)
STABILITY = 1e-06
F32 = jnp.float32
BF16 = jnp.bfloat16


def plan(number):
    current = CUMULATIVE_ALPHA[number]
    following = CUMULATIVE_ALPHA[number + 1]
    spread = 0.3 * math.sqrt(1.0 - following)
    return (
        math.sqrt(current),
        math.sqrt(1.0 - current),
        math.sqrt(following),
        math.sqrt(1.0 - following - spread * spread),
        spread,
    )


def mm(a, b):
    return jnp.dot(a, b, preferred_element_type=F32)


def mm_nt(a, b):
    return lax.dot_general(a, b, (((1,), (1,)), ((), ())), preferred_element_type=F32)


def silu_pair(v):
    s = 0.5 * jnp.tanh(0.5 * v) + 0.5
    a = v * s
    return a, s + a * (1.0 - s)


def silu_half(u):
    t = jnp.tanh(u)
    a = u * (t + 1.0)
    low, act = t.astype(BF16), a.astype(BF16)
    return u, a, (low + 1.0) + act * (1.0 - low)


def kernel(
    n, steps, per_dev, channels, height, width, hid, feat,
    latent_hbm, noise_hbm, offsets_hbm, anchors_hbm, guidance_hbm,
    w_in_hbm, w_mid_hbm, w_out_hbm, t_embed_hbm, w_feat_hbm,
    out_ref,
    latent_ref, noise_ref, offsets_ref, anchors_ref, guidance_ref,
    w_in_ref, w_mid_ref, w_out_ref, t_embed_ref, w_feat_ref, load_sem,
    wi, wit, wo, wot, wm, wmt, wfb,
    taps, outward, deriv_h, deriv_m, clean_ref, per_a, per_d, dclean_ref,
    init_src, init_dst, cover_src, cover_dst,
    anchor_buf, square_buf, own_base, own_base_in, spill_base, spill_base_in,
    own_grad, own_grad_in, spill_grad, spill_grad_in,
    init_send, init_recv, anchor_send, anchor_recv, square_send, square_recv, edge_send, edge_recv,
):
    me = lax.axis_index("wa")
    right, left = lax.rem(me + 1, n), lax.rem(me + n - 1, n)
    rows = per_dev * channels
    flat = height * width
    nine = len(TAP_SHIFTS)

    barrier = pltpu.get_barrier_semaphore()

    def greet(d, carry):
        pl.semaphore_signal(
            barrier, inc=1, device_id={"wa": lax.rem(me + d, n)},
            device_id_type=pl.DeviceIdType.MESH,
        )
        return carry

    lax.fori_loop(1, n, greet, 0)

    loads = [
        pltpu.make_async_copy(src, dst, load_sem.at[k])
        for k, (src, dst) in enumerate(
            (
                (latent_hbm, latent_ref),
                (noise_hbm, noise_ref),
                (offsets_hbm, offsets_ref),
                (w_mid_hbm, w_mid_ref),
                (w_in_hbm, w_in_ref),
                (w_out_hbm, w_out_ref),
                (t_embed_hbm, t_embed_ref),
                (w_feat_hbm, w_feat_ref),
                (anchors_hbm, anchors_ref),
                (guidance_hbm, guidance_ref),
            )
        )
    ]
    for load in loads:
        load.start()
    for load in loads[:3]:
        load.wait()

    def remote(src, dst, send_sem, recv_sem, target):
        return pltpu.make_async_remote_copy(
            src_ref=src, dst_ref=dst, send_sem=send_sem, recv_sem=recv_sem,
            device_id={"wa": target}, device_id_type=pl.DeviceIdType.MESH,
        )

    def to_all(buf, send_sem, recv_sem):
        def one(d, carry):
            remote(buf.at[0], buf.at[d], send_sem, recv_sem, lax.rem(me + d, n)).start()
            return carry

        lax.fori_loop(1, n, one, 0)

    def await_all(buf, sem):
        rest = buf.at[pl.ds(1, n - 1)]
        pltpu.make_async_copy(rest, rest, sem).wait()

    lane = lax.broadcasted_iota(jnp.int32, (rows, width), 1)
    row = lax.broadcasted_iota(jnp.int32, (rows, width), 0)
    first = row < channels
    starts = [offsets_ref[i] + i * STRIDE for i in range(per_dev)]

    ones = jnp.where(lax.broadcasted_iota(jnp.int32, (rows, flat), 0) < 3, 1.0, 0.0)

    def tiles(value):
        return [value[:, h * width : (h + 1) * width] for h in range(height)]

    def joined_tiles(parts):
        return jnp.concatenate(parts, axis=1)

    def from_right(x):
        return jnp.where(lane == width - 1, 0.0, pltpu.roll(x, width - 1, 1))

    def from_left(x):
        return jnp.where(lane == 0, 0.0, pltpu.roll(x, 1, 1))

    def expand(parts, sign):
        moved = {0: parts, 1: [from_right(p) for p in parts], -1: [from_left(p) for p in parts]}
        zero = jnp.zeros((rows, width), F32)
        blocks = []
        for down, across in TAP_SHIFTS:
            source = moved[sign * across]
            blocks.append(
                joined_tiles(
                    [
                        source[h + sign * down] if 0 <= h + sign * down < height else zero
                        for h in range(height)
                    ]
                )
            )
        blocks.append(ones)
        return jnp.concatenate(blocks, axis=0).astype(BF16)

    def collapse(ref, sign):
        result = []
        for h in range(height):
            sums = {}
            for k, (down, across) in enumerate(TAP_SHIFTS):
                source = h + sign * down
                if 0 <= source < height:
                    piece = ref[k * rows : (k + 1) * rows, source * width : (source + 1) * width]
                    key = sign * across
                    sums[key] = sums[key] + piece if key in sums else piece
            result.append(sums[0] + from_right(sums[1]) + from_left(sums[-1]))
        return result

    def half_swap(x):
        return pltpu.roll(x, channels, 0)

    for h in range(height):
        cols = slice(h * width, (h + 1) * width)
        init_src[0:channels, cols] = latent_ref[:, h, :]
        for s in range(steps - 1):
            init_src[(s + 1) * channels : (s + 2) * channels, cols] = noise_ref[s, :, h, :]
    own_cover = jnp.zeros((rows, width), F32)
    for i in range(per_dev):
        own_cover = own_cover + (lane >= starts[i]).astype(F32)
    spill_cover = per_dev - own_cover
    cover_src[0] = own_cover
    cover_src[1] = spill_cover

    pl.semaphore_wait(barrier, n - 1)
    init_copy = remote(init_src, init_dst, init_send.at[0], init_recv.at[0], left)
    cover_left = remote(cover_src.at[0], cover_dst.at[0], init_send.at[1], init_recv.at[1], left)
    cover_right = remote(cover_src.at[1], cover_dst.at[1], init_send.at[2], init_recv.at[2], right)
    init_copy.start()
    cover_left.start()
    cover_right.start()

    for load in loads[3:]:
        load.wait()

    w_in_t = w_in_ref[...]
    w_out = w_out_ref[...]
    small = nine * channels
    eye_r = lax.broadcasted_iota(jnp.int32, (hid, hid), 0)
    eye_c = lax.broadcasted_iota(jnp.int32, (hid, hid), 1)
    eye = eye_r == eye_c
    eye_b = jnp.where(eye, 1.0, 0.0).astype(BF16)
    wm[...] = (0.5 * w_mid_ref[...].astype(F32)).astype(BF16)
    wmt[...] = (0.25 * mm_nt(eye_b, w_mid_ref[...])).astype(BF16)
    w_out_t = mm_nt(eye_b, w_out).astype(BF16)
    w_in = mm_nt(eye_b, w_in_t).astype(BF16)
    place = lax.broadcasted_iota(jnp.int32, (hid, (nine + 1) * rows), 1)
    embeds = []
    for s in range(steps):
        rest = 0.5 * jnp.sum(jnp.where(eye, t_embed_ref[s : s + 1, :], 0.0), axis=1, keepdims=True)
        spread_out = jnp.zeros((hid, (nine + 1) * rows), F32)
        for k in range(3):
            term = rest.astype(BF16).astype(F32)
            spread_out = jnp.where(place == nine * rows + k, term, spread_out)
            rest = rest - term
        embeds.append(spread_out)
    for i in range(per_dev):
        def hot(a, b):
            return jnp.where((a // channels) * rows + i * channels + a % channels == b, 1.0, 0.0).astype(BF16)

        spot = hot(
            lax.broadcasted_iota(jnp.int32, (small, (nine + 1) * rows), 0),
            lax.broadcasted_iota(jnp.int32, (small, (nine + 1) * rows), 1),
        )
        spot_t = hot(
            lax.broadcasted_iota(jnp.int32, (nine * rows, small), 1),
            lax.broadcasted_iota(jnp.int32, (nine * rows, small), 0),
        )
        taken = 0.5 * mm(w_in, spot)
        for s in range(steps):
            wi[s, i] = (taken + embeds[s]).astype(BF16)
        wit[i] = mm(spot_t, w_in_t).astype(BF16)
        wo[i] = mm(spot_t, w_out).astype(BF16)
        wot[i] = mm(w_out_t, spot).astype(BF16)
    for c in range(channels):
        column = jnp.sum(
            jnp.where(eye[0:feat, 0:feat], w_feat_ref[c : c + 1, :], 0.0), axis=1, keepdims=True
        )
        wfb[c] = jnp.broadcast_to(column, (feat, width))

    cover_left.wait()
    cover_right.wait()
    count_own = own_cover + cover_dst[1]
    count_next = cover_dst[0] + spill_cover
    init_copy.wait()

    def all_tiles(count):
        return jnp.concatenate([count[0:channels]] * height, axis=1)

    def doubled(value):
        return jnp.concatenate([value] * per_dev, axis=0)

    state = tiles(doubled(init_src[0:channels, :]))
    state_next = tiles(doubled(init_dst[0:channels, :]))

    for s in range(steps):
        now_a, now_s, next_a, direction, spread = plan(s)
        last = s == steps - 1
        slot = lax.rem(anchors_ref[s], per_dev)
        owner = lax.div(anchors_ref[s], per_dev)
        order = [jnp.where(slot == 0, starts[0], starts[1]), jnp.where(slot == 0, starts[1], starts[0])]
        keep = lane >= jnp.where(first, order[0], order[1])

        window = []
        for h in range(height):
            cut = [
                pltpu.roll(jnp.where(lane >= start, state[h], state_next[h]), width - start, 1)
                for start in order
            ]
            window.append(jnp.where(first, cut[0], cut[1]))
        taps[...] = expand(window, 1)

        def forward(i):
            def block(j, carry):
                for part in range(SIDE):
                    cols = pl.ds(pl.multiple_of((j * SIDE + part) * CHUNK, CHUNK), CHUNK)
                    stacked = taps[:, cols]
                    half, act, slope = silu_half(mm(wi[s, i], stacked))
                    act = act.astype(BF16)
                    deriv_h[i, :, cols] = slope
                    act2, slope2 = silu_half(mm(wm[...], act))[1:]
                    deriv_m[i, :, cols] = slope2
                    piece = mm(wo[i], ((half + half) + act2).astype(BF16))
                    outward[:, cols] = piece if i == 0 else outward[:, cols] + piece
                return carry

            lax.fori_loop(0, flat // (CHUNK * SIDE), block, 0)
            predicted = collapse(outward, 1)
            cleaned = [(window[h] - now_s * predicted[h]) * (1.0 / now_a) for h in range(height)]
            return predicted, cleaned

        cleaned = forward(0)[1]
        anchor_buf[s, 0] = jnp.where(owner == me, joined_tiles(cleaned)[0:channels, :], 0.0)
        to_all(anchor_buf.at[s], anchor_send.at[s], anchor_recv.at[s])
        predicted, cleaned = forward(1)
        clean_all = joined_tiles(cleaned)
        clean_ref[...] = clean_all

        def percept_of(source, base):
            value = wfb[0] * source[base : base + 1, :]
            for c in range(1, channels):
                value = value + wfb[c] * source[base + c : base + c + 1, :]
            return value

        def features(h, carry):
            cols = pl.ds(pl.multiple_of(h * width, width), width)
            source = clean_ref[:, cols]
            for i in range(per_dev):
                act, slope = silu_pair(percept_of(source, i * channels))
                per_a[i, :, cols] = act
                per_d[i, :, cols] = slope
            return carry

        lax.fori_loop(0, height, features, 0)

        def placed(x):
            moved = jnp.where(first, pltpu.roll(x, order[0], 1), pltpu.roll(x, order[1], 1))
            own = jnp.where(keep, moved, 0.0)
            over = moved - own
            return (own + half_swap(own))[0:channels], (over + half_swap(over))[0:channels]

        def share(parts, own, own_in, spill, spill_in, at):
            pairs = [placed(p) for p in parts]
            spill[s] = joined_tiles([p[1] for p in pairs])
            to_right = remote(spill.at[s], spill_in.at[s], edge_send.at[s, at], edge_recv.at[s, at], right)
            to_right.start()
            own[s] = joined_tiles([p[0] for p in pairs])
            if last:
                return [to_right]
            to_left = remote(own.at[s], own_in.at[s], edge_send.at[s, at + 1], edge_recv.at[s, at + 1], left)
            to_left.start()
            return [to_right, to_left]

        base = [
            (next_a / now_a) * (window[h] - now_s * predicted[h]) + direction * predicted[h]
            for h in range(height)
        ]
        edges = share(base, own_base, own_base_in, spill_base, spill_base_in, 0)

        await_all(anchor_buf.at[s], anchor_recv.at[s])

        def backward_features(h, carry):
            cols = pl.ds(pl.multiple_of(h * width, width), width)
            anchor = anchor_buf[s, 0, :, cols]
            for d in range(1, n):
                anchor = anchor + anchor_buf[s, d, :, cols]
            anchor_act = silu_pair(percept_of(anchor, 0))[0]
            lines = []
            for i in range(per_dev):
                slope = (per_a[i, :, cols] - anchor_act) * (1.0 / feat) * per_d[i, :, cols]
                for c in range(channels):
                    lines.append(jnp.sum(wfb[c] * slope, axis=0, keepdims=True))
            dclean_ref[:, cols] = jnp.concatenate(lines, axis=0)
            return carry

        lax.fori_loop(0, height, backward_features, 0)

        dclean = tiles(dclean_ref[...])
        taps[...] = expand([(-now_s / now_a) * d for d in dclean], -1)

        def backward(j, carry):
            cols = pl.ds(pl.multiple_of(j * CHUNK, CHUNK), CHUNK)
            stacked = taps[:, cols]
            total = None
            for i in range(per_dev):
                d_joined = mm(wot[i], stacked).astype(BF16)
                d_act = mm(wmt[...], d_joined * deriv_m[i, :, cols]).astype(BF16)
                d_hidden = d_joined + d_act * deriv_h[i, :, cols]
                piece = mm(wit[i], d_hidden)
                total = piece if total is None else total + piece
            outward[:, cols] = total.astype(BF16).astype(F32)
            return carry

        lax.fori_loop(0, flat // CHUNK, backward, 0)

        through = collapse(outward, -1)
        gradient = [
            dclean[h] * (1.0 / now_a) + through[h].astype(BF16).astype(F32) for h in range(height)
        ]
        square = gradient[0] * gradient[0]
        for h in range(1, height):
            square = square + gradient[h] * gradient[h]
        square_buf[s, 0] = square
        to_all(square_buf.at[s], square_send.at[s], square_recv.at[s])

        edges += share(gradient, own_grad, own_grad_in, spill_grad, spill_grad_in, 2)

        def merged(base, grad, coef, count, noise):
            return (base - coef * grad) / all_tiles(count) + spread * noise

        await_all(square_buf.at[s], square_recv.at[s])
        square = square_buf[s, 0]
        for d in range(1, n):
            square = square + square_buf[s, d]
        mean = jnp.sum(jnp.sum(square, axis=0, keepdims=True), axis=1, keepdims=True) * (
            1.0 / (n * rows * flat)
        )
        coef = (next_a / now_a) * guidance_ref[0] * lax.rsqrt(
            jnp.broadcast_to(mean, (channels, flat)) + STABILITY
        )
        for edge in edges:
            edge.wait()
        block = merged(
            own_base[s] + spill_base_in[s], own_grad[s] + spill_grad_in[s], coef, count_own,
            0.0 if last else init_src[(s + 1) * channels : (s + 2) * channels, :],
        )
        if last:
            for h in range(height):
                out_ref[:, h, :] = block[:, h * width : (h + 1) * width] + spread * noise_ref[s, :, h, :]
        else:
            beyond = merged(
                own_base_in[s] + spill_base[s], own_grad_in[s] + spill_grad[s], coef, count_next,
                init_dst[(s + 1) * channels : (s + 2) * channels, :],
            )
            state = tiles(doubled(block))
            state_next = tiles(doubled(beyond))

    for s in range(steps):
        await_all(anchor_buf.at[s], anchor_send.at[s])
        await_all(square_buf.at[s], square_send.at[s])


def local(n, latent, noise, offsets, anchors, guidance, w_in, w_mid, w_out, t_embed, w_feat):
    channels, height, width = latent.shape
    per_dev = offsets.shape[0]
    steps = t_embed.shape[0]
    hid = w_mid.shape[0]
    feat = w_feat.shape[0]
    rows = per_dev * channels
    assert width == WIN and per_dev == 2
    flat = height * width
    tall = len(TAP_SHIFTS) * rows
    vmem = pl.BlockSpec(memory_space=pltpu.VMEM)
    hbm = pl.BlockSpec(memory_space=pltpu.HBM)
    operands = (latent, noise, offsets, anchors, guidance, w_in.T, w_mid, w_out, t_embed, w_feat.T)
    in_smem = (2, 3, 4)
    dma = pltpu.SemaphoreType.DMA
    return pl.pallas_call(
        functools.partial(kernel, n, steps, per_dev, channels, height, width, hid, feat),
        out_shape=jax.ShapeDtypeStruct(latent.shape, F32),
        in_specs=[hbm] * len(operands),
        out_specs=vmem,
        scratch_shapes=[
            (pltpu.SMEM if k in in_smem else pltpu.VMEM)(x.shape, x.dtype)
            for k, x in enumerate(operands)
        ]
        + [
            dma((len(operands),)),
            pltpu.VMEM((steps, per_dev, hid, tall + rows), BF16),
            pltpu.VMEM((per_dev, tall, hid), BF16),
            pltpu.VMEM((per_dev, tall, hid), BF16),
            pltpu.VMEM((per_dev, hid, tall + rows), BF16),
            pltpu.VMEM((hid, hid), BF16),
            pltpu.VMEM((hid, hid), BF16),
            pltpu.VMEM((channels, feat, width), F32),
            pltpu.VMEM((tall + rows, flat), BF16),
            pltpu.VMEM((tall, flat), F32),
            pltpu.VMEM((per_dev, hid, flat), BF16),
            pltpu.VMEM((per_dev, hid, flat), BF16),
            pltpu.VMEM((rows, flat), F32),
            pltpu.VMEM((per_dev, feat, flat), F32),
            pltpu.VMEM((per_dev, feat, flat), F32),
            pltpu.VMEM((rows, flat), F32),
            pltpu.VMEM((steps * channels, flat), F32),
            pltpu.VMEM((steps * channels, flat), F32),
            pltpu.VMEM((2, rows, width), F32),
            pltpu.VMEM((2, rows, width), F32),
            pltpu.VMEM((steps, n, channels, flat), F32),
            pltpu.VMEM((steps, n, rows, width), F32),
            *[pltpu.VMEM((steps, channels, flat), F32)] * 8,
            dma((3,)),
            dma((3,)),
            dma((steps,)),
            dma((steps,)),
            dma((steps,)),
            dma((steps,)),
            dma((steps, 4)),
            dma((steps, 4)),
        ],
        compiler_params=pltpu.CompilerParams(
            collective_id=0, has_side_effects=True, vmem_limit_bytes=67_000_000
        ),
        name="panorama",
    )(*operands)


def solution(mesh):
    return jax.shard_map(
        functools.partial(local, mesh.shape["wa"]),
        mesh=mesh,
        in_specs=(
            P("ba", None, "wa"),
            P(None, "ba", None, "wa"),
            P("wa"),
            P(),
            P(),
            P(),
            P(),
            P(),
            P(),
            P(),
        ),
        out_specs=P("ba", None, "wa"),
        check_vma=False,
    )
```

```python
import functools
import math

import jax
import jax.numpy as jnp
from jax import lax
from jax.experimental import pallas as pl
from jax.experimental.pallas import tpu as pltpu
from jax.sharding import PartitionSpec as P

WIN = 128
STRIDE = 64
CHUNK = 512
SIDE = 1
WIDE = 1024

TAP_SHIFTS = ((-1, -1), (-1, 0), (-1, 1), (0, -1), (0, 0), (0, 1), (1, -1), (1, 0), (1, 1))
CUMULATIVE_ALPHA = (0.35, 0.55, 0.72, 0.85, 0.93)
STABILITY = 1e-06
F32 = jnp.float32
BF16 = jnp.bfloat16


def plan(number):
    current = CUMULATIVE_ALPHA[number]
    following = CUMULATIVE_ALPHA[number + 1]
    spread = 0.3 * math.sqrt(1.0 - following)
    return (
        math.sqrt(current),
        math.sqrt(1.0 - current),
        math.sqrt(following),
        math.sqrt(1.0 - following - spread * spread),
        spread,
    )


def mm(a, b):
    return jnp.dot(a, b, preferred_element_type=F32)


def mm_nt(a, b):
    return lax.dot_general(a, b, (((1,), (1,)), ((), ())), preferred_element_type=F32)


def silu_pair(v):
    s = 0.5 * jnp.tanh(0.5 * v) + 0.5
    a = v * s
    return a, s + a * (1.0 - s)


def silu_half(u):
    t = jnp.tanh(u)
    a = u * (t + 1.0)
    low, act = t.astype(BF16), a.astype(BF16)
    return u, a, (low + 1.0) + act * (1.0 - low)


def kernel(
    n, steps, per_dev, channels, height, width, hid, feat,
    latent_hbm, noise_hbm, offsets_hbm, anchors_hbm, guidance_hbm,
    w_in_hbm, w_mid_hbm, w_out_hbm, t_embed_hbm, w_feat_hbm,
    out_ref,
    latent_ref, noise_ref, offsets_ref, anchors_ref, guidance_ref,
    w_in_ref, w_mid_ref, w_out_ref, t_embed_ref, w_feat_ref, load_sem,
    wi, wit, wo, wot, wm, wmt, wfb,
    taps, outward, second, deriv_h, deriv_m, clean_ref, per_a, per_d, dclean_ref,
    init_src, init_dst, cover_src, cover_dst,
    anchor_buf, square_buf, own_base, own_base_in, spill_base, spill_base_in,
    own_grad, own_grad_in, spill_grad, spill_grad_in,
    init_send, init_recv, anchor_send, anchor_recv, square_send, square_recv, edge_send, edge_recv,
):
    me = lax.axis_index("wa")
    right, left = lax.rem(me + 1, n), lax.rem(me + n - 1, n)
    rows = per_dev * channels
    flat = height * width
    nine = len(TAP_SHIFTS)

    barrier = pltpu.get_barrier_semaphore()

    def greet(d, carry):
        pl.semaphore_signal(
            barrier, inc=1, device_id={"wa": lax.rem(me + d, n)},
            device_id_type=pl.DeviceIdType.MESH,
        )
        return carry

    lax.fori_loop(1, n, greet, 0)

    loads = [
        pltpu.make_async_copy(src, dst, load_sem.at[k])
        for k, (src, dst) in enumerate(
            (
                (latent_hbm, latent_ref),
                (noise_hbm, noise_ref),
                (offsets_hbm, offsets_ref),
                (w_mid_hbm, w_mid_ref),
                (w_in_hbm, w_in_ref),
                (w_out_hbm, w_out_ref),
                (t_embed_hbm, t_embed_ref),
                (w_feat_hbm, w_feat_ref),
                (anchors_hbm, anchors_ref),
                (guidance_hbm, guidance_ref),
            )
        )
    ]
    for load in loads:
        load.start()
    for load in loads[:3]:
        load.wait()

    def remote(src, dst, send_sem, recv_sem, target):
        return pltpu.make_async_remote_copy(
            src_ref=src, dst_ref=dst, send_sem=send_sem, recv_sem=recv_sem,
            device_id={"wa": target}, device_id_type=pl.DeviceIdType.MESH,
        )

    def to_all(buf, send_sem, recv_sem):
        def one(d, carry):
            remote(buf.at[0], buf.at[d], send_sem, recv_sem, lax.rem(me + d, n)).start()
            return carry

        lax.fori_loop(1, n, one, 0)

    def await_all(buf, sem):
        rest = buf.at[pl.ds(1, n - 1)]
        pltpu.make_async_copy(rest, rest, sem).wait()

    lane = lax.broadcasted_iota(jnp.int32, (rows, width), 1)
    row = lax.broadcasted_iota(jnp.int32, (rows, width), 0)
    first = row < channels
    starts = [offsets_ref[i] + i * STRIDE for i in range(per_dev)]

    ones = jnp.where(lax.broadcasted_iota(jnp.int32, (rows, flat), 0) < 3, 1.0, 0.0)

    def tiles(value):
        return [value[:, h * width : (h + 1) * width] for h in range(height)]

    def joined_tiles(parts):
        return jnp.concatenate(parts, axis=1)

    def from_right(x):
        return jnp.where(lane == width - 1, 0.0, pltpu.roll(x, width - 1, 1))

    def from_left(x):
        return jnp.where(lane == 0, 0.0, pltpu.roll(x, 1, 1))

    def expand(parts, sign):
        moved = {0: parts, 1: [from_right(p) for p in parts], -1: [from_left(p) for p in parts]}
        zero = jnp.zeros((rows, width), F32)
        blocks = []
        for down, across in TAP_SHIFTS:
            source = moved[sign * across]
            blocks.append(
                joined_tiles(
                    [
                        source[h + sign * down] if 0 <= h + sign * down < height else zero
                        for h in range(height)
                    ]
                )
            )
        blocks.append(ones)
        return jnp.concatenate(blocks, axis=0).astype(BF16)

    def collapse(ref, sign):
        result = []
        for h in range(height):
            sums = {}
            for k, (down, across) in enumerate(TAP_SHIFTS):
                source = h + sign * down
                if 0 <= source < height:
                    piece = ref[k * rows : (k + 1) * rows, source * width : (source + 1) * width]
                    key = sign * across
                    sums[key] = sums[key] + piece if key in sums else piece
            result.append(sums[0] + from_right(sums[1]) + from_left(sums[-1]))
        return result

    def half_swap(x):
        return pltpu.roll(x, channels, 0)

    for h in range(height):
        cols = slice(h * width, (h + 1) * width)
        init_src[0:channels, cols] = latent_ref[:, h, :]
        for s in range(steps - 1):
            init_src[(s + 1) * channels : (s + 2) * channels, cols] = noise_ref[s, :, h, :]
    own_cover = jnp.zeros((rows, width), F32)
    for i in range(per_dev):
        own_cover = own_cover + (lane >= starts[i]).astype(F32)
    spill_cover = per_dev - own_cover
    cover_src[0] = own_cover
    cover_src[1] = spill_cover

    pl.semaphore_wait(barrier, n - 1)
    init_copy = remote(init_src, init_dst, init_send.at[0], init_recv.at[0], left)
    cover_left = remote(cover_src.at[0], cover_dst.at[0], init_send.at[1], init_recv.at[1], left)
    cover_right = remote(cover_src.at[1], cover_dst.at[1], init_send.at[2], init_recv.at[2], right)
    init_copy.start()
    cover_left.start()
    cover_right.start()

    for load in loads[3:]:
        load.wait()

    w_in_t = w_in_ref[...]
    w_out = w_out_ref[...]
    small = nine * channels
    eye_r = lax.broadcasted_iota(jnp.int32, (hid, hid), 0)
    eye_c = lax.broadcasted_iota(jnp.int32, (hid, hid), 1)
    eye = eye_r == eye_c
    eye_b = jnp.where(eye, 1.0, 0.0).astype(BF16)
    wm[...] = (0.5 * w_mid_ref[...].astype(F32)).astype(BF16)
    wmt[...] = (0.25 * mm_nt(eye_b, w_mid_ref[...])).astype(BF16)
    w_out_t = mm_nt(eye_b, w_out).astype(BF16)
    w_in = mm_nt(eye_b, w_in_t).astype(BF16)
    place = lax.broadcasted_iota(jnp.int32, (hid, (nine + 1) * rows), 1)
    embeds = []
    for s in range(steps):
        rest = 0.5 * jnp.sum(jnp.where(eye, t_embed_ref[s : s + 1, :], 0.0), axis=1, keepdims=True)
        spread_out = jnp.zeros((hid, (nine + 1) * rows), F32)
        for k in range(3):
            term = rest.astype(BF16).astype(F32)
            spread_out = jnp.where(place == nine * rows + k, term, spread_out)
            rest = rest - term
        embeds.append(spread_out)
    for i in range(per_dev):
        def hot(a, b):
            return jnp.where((a // channels) * rows + i * channels + a % channels == b, 1.0, 0.0).astype(BF16)

        spot = hot(
            lax.broadcasted_iota(jnp.int32, (small, (nine + 1) * rows), 0),
            lax.broadcasted_iota(jnp.int32, (small, (nine + 1) * rows), 1),
        )
        spot_t = hot(
            lax.broadcasted_iota(jnp.int32, (nine * rows, small), 1),
            lax.broadcasted_iota(jnp.int32, (nine * rows, small), 0),
        )
        taken = 0.5 * mm(w_in, spot)
        for s in range(steps):
            wi[s, i] = (taken + embeds[s]).astype(BF16)
        wit[i] = mm(spot_t, w_in_t).astype(BF16)
        wo[i] = mm(spot_t, w_out).astype(BF16)
        wot[i] = mm(w_out_t, spot).astype(BF16)
    for c in range(channels):
        column = jnp.sum(
            jnp.where(eye[0:feat, 0:feat], w_feat_ref[c : c + 1, :], 0.0), axis=1, keepdims=True
        )
        wfb[c] = jnp.broadcast_to(column, (feat, width))

    cover_left.wait()
    cover_right.wait()
    count_own = own_cover + cover_dst[1]
    count_next = cover_dst[0] + spill_cover
    init_copy.wait()

    def all_tiles(count):
        return jnp.concatenate([count[0:channels]] * height, axis=1)

    def doubled(value):
        return jnp.concatenate([value] * per_dev, axis=0)

    state = tiles(doubled(init_src[0:channels, :]))
    state_next = tiles(doubled(init_dst[0:channels, :]))

    for s in range(steps):
        now_a, now_s, next_a, direction, spread = plan(s)
        last = s == steps - 1
        slot = lax.rem(anchors_ref[s], per_dev)
        owner = lax.div(anchors_ref[s], per_dev)
        order = [jnp.where(slot == 0, starts[0], starts[1]), jnp.where(slot == 0, starts[1], starts[0])]
        keep = lane >= jnp.where(first, order[0], order[1])

        window = []
        for h in range(height):
            cut = [
                pltpu.roll(jnp.where(lane >= start, state[h], state_next[h]), width - start, 1)
                for start in order
            ]
            window.append(jnp.where(first, cut[0], cut[1]))
        taps[...] = expand(window, 1)

        def forward(i):
            def block(j, carry):
                for part in range(SIDE):
                    cols = pl.ds(pl.multiple_of((j * SIDE + part) * WIDE, WIDE), WIDE)
                    stacked = taps[:, cols]
                    half, act, slope = silu_half(mm(wi[s, i], stacked))
                    act = act.astype(BF16)
                    deriv_h[i, :, cols] = slope
                    act2, slope2 = silu_half(mm(wm[...], act))[1:]
                    deriv_m[i, :, cols] = slope2
                    piece = mm(wo[i], ((half + half) + act2).astype(BF16))
                    (outward if i == 0 else second)[:, cols] = piece
                return carry

            lax.fori_loop(0, flat // (WIDE * SIDE), block, 0)
            predicted = collapse(outward, 1)
            if i == 1:
                late = collapse(second, 1)
                predicted = [jnp.where(first, p, q) for p, q in zip(predicted, late)]
            cleaned = [(window[h] - now_s * predicted[h]) * (1.0 / now_a) for h in range(height)]
            return predicted, cleaned

        cleaned = forward(0)[1]
        anchor_buf[s, 0] = jnp.where(owner == me, joined_tiles(cleaned)[0:channels, :], 0.0)
        to_all(anchor_buf.at[s], anchor_send.at[s], anchor_recv.at[s])
        predicted, cleaned = forward(1)
        clean_all = joined_tiles(cleaned)
        clean_ref[...] = clean_all

        def percept_of(source, base):
            value = wfb[0] * source[base : base + 1, :]
            for c in range(1, channels):
                value = value + wfb[c] * source[base + c : base + c + 1, :]
            return value

        def features(h, carry):
            cols = pl.ds(pl.multiple_of(h * width, width), width)
            source = clean_ref[:, cols]
            for i in range(per_dev):
                act, slope = silu_pair(percept_of(source, i * channels))
                per_a[i, :, cols] = act
                per_d[i, :, cols] = slope
            return carry

        lax.fori_loop(0, height, features, 0)

        def placed(x):
            moved = jnp.where(first, pltpu.roll(x, order[0], 1), pltpu.roll(x, order[1], 1))
            own = jnp.where(keep, moved, 0.0)
            over = moved - own
            return (own + half_swap(own))[0:channels], (over + half_swap(over))[0:channels]

        def share(parts, own, own_in, spill, spill_in, at):
            pairs = [placed(p) for p in parts]
            spill[s] = joined_tiles([p[1] for p in pairs])
            to_right = remote(spill.at[s], spill_in.at[s], edge_send.at[s, at], edge_recv.at[s, at], right)
            to_right.start()
            own[s] = joined_tiles([p[0] for p in pairs])
            if last:
                return [to_right]
            to_left = remote(own.at[s], own_in.at[s], edge_send.at[s, at + 1], edge_recv.at[s, at + 1], left)
            to_left.start()
            return [to_right, to_left]

        base = [
            (next_a / now_a) * (window[h] - now_s * predicted[h]) + direction * predicted[h]
            for h in range(height)
        ]
        edges = share(base, own_base, own_base_in, spill_base, spill_base_in, 0)

        await_all(anchor_buf.at[s], anchor_recv.at[s])

        def backward_features(h, carry):
            cols = pl.ds(pl.multiple_of(h * width, width), width)
            anchor = anchor_buf[s, 0, :, cols]
            for d in range(1, n):
                anchor = anchor + anchor_buf[s, d, :, cols]
            anchor_act = silu_pair(percept_of(anchor, 0))[0]
            lines = []
            for i in range(per_dev):
                slope = (per_a[i, :, cols] - anchor_act) * (1.0 / feat) * per_d[i, :, cols]
                for c in range(channels):
                    lines.append(jnp.sum(wfb[c] * slope, axis=0, keepdims=True))
            dclean_ref[:, cols] = jnp.concatenate(lines, axis=0)
            return carry

        lax.fori_loop(0, height, backward_features, 0)

        dclean = tiles(dclean_ref[...])
        taps[...] = expand([(-now_s / now_a) * d for d in dclean], -1)

        def backward(j, carry):
            cols = pl.ds(pl.multiple_of(j * CHUNK, CHUNK), CHUNK)
            stacked = taps[:, cols]
            total = None
            for i in range(per_dev):
                d_joined = mm(wot[i], stacked).astype(BF16)
                d_act = mm(wmt[...], d_joined * deriv_m[i, :, cols]).astype(BF16)
                d_hidden = d_joined + d_act * deriv_h[i, :, cols]
                piece = mm(wit[i], d_hidden)
                total = piece if total is None else total + piece
            outward[:, cols] = total.astype(BF16).astype(F32)
            return carry

        lax.fori_loop(0, flat // CHUNK, backward, 0)

        through = collapse(outward, -1)
        gradient = [
            dclean[h] * (1.0 / now_a) + through[h].astype(BF16).astype(F32) for h in range(height)
        ]
        square = gradient[0] * gradient[0]
        for h in range(1, height):
            square = square + gradient[h] * gradient[h]
        square_buf[s, 0] = square
        to_all(square_buf.at[s], square_send.at[s], square_recv.at[s])

        edges += share(gradient, own_grad, own_grad_in, spill_grad, spill_grad_in, 2)

        def merged(base, grad, coef, count, noise):
            return (base - coef * grad) / all_tiles(count) + spread * noise

        await_all(square_buf.at[s], square_recv.at[s])
        square = square_buf[s, 0]
        for d in range(1, n):
            square = square + square_buf[s, d]
        mean = jnp.sum(jnp.sum(square, axis=0, keepdims=True), axis=1, keepdims=True) * (
            1.0 / (n * rows * flat)
        )
        coef = (next_a / now_a) * guidance_ref[0] * lax.rsqrt(
            jnp.broadcast_to(mean, (channels, flat)) + STABILITY
        )
        for edge in edges:
            edge.wait()
        block = merged(
            own_base[s] + spill_base_in[s], own_grad[s] + spill_grad_in[s], coef, count_own,
            0.0 if last else init_src[(s + 1) * channels : (s + 2) * channels, :],
        )
        if last:
            for h in range(height):
                out_ref[:, h, :] = block[:, h * width : (h + 1) * width] + spread * noise_ref[s, :, h, :]
        else:
            beyond = merged(
                own_base_in[s] + spill_base[s], own_grad_in[s] + spill_grad[s], coef, count_next,
                init_dst[(s + 1) * channels : (s + 2) * channels, :],
            )
            state = tiles(doubled(block))
            state_next = tiles(doubled(beyond))

    for s in range(steps):
        await_all(anchor_buf.at[s], anchor_send.at[s])
        await_all(square_buf.at[s], square_send.at[s])


def local(n, latent, noise, offsets, anchors, guidance, w_in, w_mid, w_out, t_embed, w_feat):
    channels, height, width = latent.shape
    per_dev = offsets.shape[0]
    steps = t_embed.shape[0]
    hid = w_mid.shape[0]
    feat = w_feat.shape[0]
    rows = per_dev * channels
    assert width == WIN and per_dev == 2
    flat = height * width
    tall = len(TAP_SHIFTS) * rows
    vmem = pl.BlockSpec(memory_space=pltpu.VMEM)
    hbm = pl.BlockSpec(memory_space=pltpu.HBM)
    operands = (latent, noise, offsets, anchors, guidance, w_in.T, w_mid, w_out, t_embed, w_feat.T)
    in_smem = (2, 3, 4)
    dma = pltpu.SemaphoreType.DMA
    return pl.pallas_call(
        functools.partial(kernel, n, steps, per_dev, channels, height, width, hid, feat),
        out_shape=jax.ShapeDtypeStruct(latent.shape, F32),
        in_specs=[hbm] * len(operands),
        out_specs=vmem,
        scratch_shapes=[
            (pltpu.SMEM if k in in_smem else pltpu.VMEM)(x.shape, x.dtype)
            for k, x in enumerate(operands)
        ]
        + [
            dma((len(operands),)),
            pltpu.VMEM((steps, per_dev, hid, tall + rows), BF16),
            pltpu.VMEM((per_dev, tall, hid), BF16),
            pltpu.VMEM((per_dev, tall, hid), BF16),
            pltpu.VMEM((per_dev, hid, tall + rows), BF16),
            pltpu.VMEM((hid, hid), BF16),
            pltpu.VMEM((hid, hid), BF16),
            pltpu.VMEM((channels, feat, width), F32),
            pltpu.VMEM((tall + rows, flat), BF16),
            pltpu.VMEM((tall, flat), F32),
            pltpu.VMEM((tall, flat), F32),
            pltpu.VMEM((per_dev, hid, flat), BF16),
            pltpu.VMEM((per_dev, hid, flat), BF16),
            pltpu.VMEM((rows, flat), F32),
            pltpu.VMEM((per_dev, feat, flat), F32),
            pltpu.VMEM((per_dev, feat, flat), F32),
            pltpu.VMEM((rows, flat), F32),
            pltpu.VMEM((steps * channels, flat), F32),
            pltpu.VMEM((steps * channels, flat), F32),
            pltpu.VMEM((2, rows, width), F32),
            pltpu.VMEM((2, rows, width), F32),
            pltpu.VMEM((steps, n, channels, flat), F32),
            pltpu.VMEM((steps, n, rows, width), F32),
            *[pltpu.VMEM((steps, channels, flat), F32)] * 8,
            dma((3,)),
            dma((3,)),
            dma((steps,)),
            dma((steps,)),
            dma((steps,)),
            dma((steps,)),
            dma((steps, 4)),
            dma((steps, 4)),
        ],
        compiler_params=pltpu.CompilerParams(
            collective_id=0, has_side_effects=True, vmem_limit_bytes=67_000_000
        ),
        name="panorama",
    )(*operands)


def solution(mesh):
    return jax.shard_map(
        functools.partial(local, mesh.shape["wa"]),
        mesh=mesh,
        in_specs=(
            P("ba", None, "wa"),
            P(None, "ba", None, "wa"),
            P("wa"),
            P(),
            P(),
            P(),
            P(),
            P(),
            P(),
            P(),
        ),
        out_specs=P("ba", None, "wa"),
        check_vma=False,
    )
```
